512 devices in a mesh: rows: 512 (over z, y, x, core).
Axes of the slice: x: 4, y: 8, z: 8, core: 2. Of those that a mesh axis runs over, the one named last changes fastest.
Arguments:
- adj_diag: int32 [8192, 512], P('rows'), may hold values from -2147483648 to 2147483647
- adj_right: int32 [8192, 512], P('rows'), may hold values from -2147483648 to 2147483647
- alive_diag: int32 [8192, 512], P('rows'), may hold values from -2147483648 to 2147483647
- alive_right: int32 [8192, 512], P('rows'), may hold values from -2147483648 to 2147483647
- truss_k: int32 [1], replicated, may hold values from 130 to 193
Outputs:
- support_field: float32 [262144, 1024], P('rows')
- removed_counts: int32 [3], replicated
The draws below stay inside these ranges and needn't reach their ends.
All inputs are finite; a program needn't handle non-finite values.
Results may differ from the reference program's by a relative error of at most 0.0003.
Values may be sent and summed in bfloat16 or wider, within the bound.
A program may use at most 64 MiB of HBM per device.

```python
import jax
import jax.numpy as jnp
from jax import lax

TILE = 512
ITERS = 3
NVERT = 262144


def vertex_levels(key, block):
    base_key = jax.random.fold_in(jax.random.fold_in(key, 7001), block)
    size_key, order_key, level_key = jax.random.split(base_key, 3)
    core_count = jax.random.randint(size_key, (), TILE // 4, 3 * TILE // 8 + 1, dtype=jnp.int32)
    order = jax.random.permutation(order_key, TILE)
    is_core = order < core_count
    levels = jax.random.randint(level_key, (TILE,), 2, 16, dtype=jnp.int32)
    return (jnp.where(is_core, jnp.int32(16), levels), is_core)


def pack_bits(tile_bits):
    shifts = jnp.arange(32, dtype=jnp.int32)
    sectioned = tile_bits.reshape(TILE // 32, 32, TILE)
    return jnp.sum(sectioned << shifts[None, :, None], axis=1, dtype=jnp.int32)


def draw_bits(key, salt, offset, alive_kind):
    blocks = NVERT // TILE

    def one_block(block):
        row_levels, row_core = vertex_levels(key, block)
        col_levels, col_core = vertex_levels(key, (block + offset) % blocks)
        edge_key = jax.random.fold_in(jax.random.fold_in(key, salt), block)
        if alive_kind:
            chance = jax.random.randint(edge_key, (TILE, TILE), 0, 8, dtype=jnp.int32)
            both_core = row_core[:, None] & col_core[None, :]
            tile_bits = jnp.where(both_core, jnp.int32(1), (chance < 7).astype(jnp.int32))
        else:
            chance = jax.random.randint(edge_key, (TILE, TILE), 0, 256, dtype=jnp.int32)
            tile_bits = (chance < row_levels[:, None] * col_levels[None, :]).astype(jnp.int32)
        return pack_bits(tile_bits)
    packed = lax.map(one_block, jnp.arange(blocks, dtype=jnp.int32))
    return packed.reshape(NVERT // 32, TILE)


def draw_adj_diag(key, part):
    return draw_bits(key, 101, 0, False)


def draw_adj_right(key, part):
    return draw_bits(key, 102, 1, False)


def draw_alive_diag(key, part):
    return draw_bits(key, 103, 0, True)


def draw_alive_right(key, part):
    return draw_bits(key, 104, 1, True)


def setup_inputs(seed: int = 0) -> dict:
    seeds = jax.random.split(jax.random.key(seed), 6)
    adj_diag = draw_adj_diag(jax.random.fold_in(seeds[5], 71), 0)
    adj_right = draw_adj_right(jax.random.fold_in(seeds[5], 71), 0)
    alive_diag = draw_alive_diag(jax.random.fold_in(seeds[5], 71), 0)
    alive_right = draw_alive_right(jax.random.fold_in(seeds[5], 71), 0)
    truss_k = jax.random.randint(seeds[4], (1,), TILE // 4 + 2, 3 * TILE // 8 + 2).astype(jnp.int32)
    return {"adj_diag": adj_diag, "adj_right": adj_right, "alive_diag": alive_diag, "alive_right": alive_right, "truss_k": truss_k}


def unpack_tiles(packed, blocks, tile):
    shifts = jnp.arange(32, dtype=jnp.int32)
    sectioned = packed.reshape(blocks, tile // 32, tile)
    tile_bits = (sectioned[:, :, None, :] >> shifts[None, None, :, None]) & 1
    return tile_bits.reshape(blocks, tile, tile)


def tile_support(pieces):
    within, across, prev_across, next_within = pieces
    inside = lax.dot_general(prev_across, prev_across, (((0,), (0,)), ((), ())), preferred_element_type=jnp.float32)
    inside = inside + jnp.dot(within, within, preferred_element_type=jnp.float32)
    inside = inside + lax.dot_general(across, across, (((1,), (1,)), ((), ())), preferred_element_type=jnp.float32)
    between = jnp.dot(within, across, preferred_element_type=jnp.float32)
    between = between + jnp.dot(across, next_within, preferred_element_type=jnp.float32)
    return inside, between


def reference(adj_diag, adj_right, alive_diag, alive_right, truss_k):
    blocks = NVERT // TILE
    upper_half = jnp.triu(unpack_tiles(adj_diag & alive_diag, blocks, TILE), 1)
    within = (upper_half + jnp.swapaxes(upper_half, 1, 2)).astype(jnp.bfloat16)
    across = unpack_tiles(adj_right & alive_right, blocks, TILE).astype(jnp.bfloat16)
    thresh = (truss_k[0] - 2).astype(jnp.float32)
    counts = []
    for step in range(ITERS):
        prev_across = jnp.roll(across, 1, axis=0)
        next_within = jnp.roll(within, -1, axis=0)
        inside, between = lax.map(tile_support, (within, across, prev_across, next_within))
        new_within = jnp.where(inside >= thresh, within, jnp.zeros_like(within))
        new_across = jnp.where(between >= thresh, across, jnp.zeros_like(across))
        lost_within = jnp.sum((within - new_within).astype(jnp.int32)) // 2
        lost_across = jnp.sum((across - new_across).astype(jnp.int32))
        counts.append(lost_within + lost_across)
        within, across = new_within, new_across
    support = jnp.concatenate([inside * within.astype(jnp.float32), between * across.astype(jnp.float32)], axis=2)
    return support.reshape(NVERT, 2 * TILE), jnp.stack(counts).astype(jnp.int32)
```

```python
import functools

import jax
import jax.numpy as jnp
from jax import lax
from jax.experimental import pallas as pl
from jax.experimental.pallas import tpu as pltpu
from jax.sharding import PartitionSpec as P

F8 = jnp.float8_e4m3fn
F32 = jnp.float32
WORD = 32
ITERS = 3
ROW = 16


def dot_nt(lhs, rhs):
    return lax.dot_general(lhs, rhs, (((1,), (1,)), ((), ())), preferred_element_type=F32)


def dot_nn(lhs, rhs):
    return lax.dot_general(lhs, rhs, (((1,), (0,)), ((), ())), preferred_element_type=F32)


def send(src, dst, send_sem, recv_sem, target):
    return pltpu.make_async_remote_copy(
        src_ref=src,
        dst_ref=dst,
        send_sem=send_sem,
        recv_sem=recv_sem,
        device_id=(target,),
        device_id_type=pl.DeviceIdType.MESH,
    )


def greet(barrier, target):
    pl.semaphore_signal(
        barrier, inc=1, device_id=(target,), device_id_type=pl.DeviceIdType.MESH
    )


def set_eye(eye):
    half = eye.shape[0]
    row_id = lax.broadcasted_iota(jnp.int32, (half, half), 0)
    col_id = lax.broadcasted_iota(jnp.int32, (half, half), 1)
    eye[...] = jnp.where(row_id == col_id, 1.0, 0.0).astype(F32).astype(F8)


def turned(eye, block):
    return dot_nt(eye[...], block)


def transpose(eye, src, dst):
    half = eye.shape[0]
    lo, hi = pl.ds(0, half), pl.ds(half, half)
    for i in (lo, hi):
        for j in (lo, hi):
            dst[i, j] = turned(eye, src[j, i]).astype(F8)


def bits_of(row, shift):
    return (jnp.broadcast_to(row, (WORD, row.shape[1])) >> shift[:, : row.shape[1]]) & 1


def as_f8(bits):
    return bits.astype(F32).astype(F8)


def unpack_across(src, *dsts):
    words, t = src.shape
    shift = lax.broadcasted_iota(jnp.int32, (WORD, t), 0)
    for w in range(words):
        bits = as_f8(bits_of(src[w : w + 1, :], shift))
        for dst in dsts:
            dst[pl.ds(WORD * w, WORD), :] = bits


def unpack_within(src, eye, tri, *dsts):
    words, t = src.shape
    half = t // 2
    shift = lax.broadcasted_iota(jnp.int32, (WORD, half), 0)
    ahead = lax.broadcasted_iota(jnp.int32, (WORD, half), 1) - shift
    lo, hi = pl.ds(0, half), pl.ds(half, half)
    for w in range(words):
        rows = pl.ds(WORD * w, WORD)
        top = 2 * w < words
        part = slice(0, half) if top else slice(half, t)
        bits = bits_of(src[w : w + 1, part], shift)
        first = WORD * w if top else WORD * w - half
        tri[rows, :] = as_f8(jnp.where(ahead > first, bits, 0))
        if top:
            bits = as_f8(bits_of(src[w : w + 1, half:], shift))
            for dst in dsts:
                dst[rows, hi] = bits
    for i in (lo, hi):
        both = (turned(eye, tri[i, :]) + tri[i, :].astype(F32)).astype(F8)
        for dst in dsts:
            dst[i, i] = both
    corner = turned(eye, dsts[0][lo, hi]).astype(F8)
    for dst in dsts:
        dst[hi, lo] = corner


def keep(support, thresh, old):
    old = old.astype(F32)
    return old, jnp.where(support >= thresh, old, 0.0)


def total(values):
    t = values.shape[0]
    lanes = jnp.sum(values, axis=0, keepdims=True)
    return sum(lanes[:, i : i + 128] for i in range(0, t, 128))


def removed(old_w, new_w, old_a, new_a):
    return total((old_w - new_w) + 2.0 * (old_a - new_a))


def first(
    n, k_ref, ad_ref, ar_ref, ld_ref, lr_ref,
    late, hm_out, w1_out, am_out, w0_out, a0_out, next_out, cnt_out,
    k_smem, raw, own, halo, h1, v, vm, at, atm, eye, tri, psum_in, psum_btw,
    k_sem, raw_sems, send_sems, recv_sems,
):
    words, t = ad_ref.shape
    half = t // 2
    me = lax.axis_index("rows")
    barrier = pltpu.get_barrier_semaphore()
    near = {by: lax.rem(me + by + n, n) for by in (1, -1, 2, -2)}
    for target in near.values():
        greet(barrier, target)
    loads = [
        pltpu.make_async_copy(src, raw.at[i], raw_sems.at[i])
        for i, src in enumerate((ad_ref, ar_ref, ld_ref, lr_ref))
    ]
    for load in loads:
        load.start()
    k_load = pltpu.make_async_copy(k_ref, k_smem, k_sem)
    k_load.start()
    for load in loads:
        load.wait()
    own[0] = raw[0] & raw[2]
    own[1] = raw[1] & raw[3]
    set_eye(eye)
    pl.semaphore_wait(barrier, 4)

    low = words // 2
    copies = {}
    sem = 0
    for slot, what, by in ((3, 0, -1), (2, 1, 1), (1, 0, 1), (5, 0, -2), (0, 1, 2), (4, 1, -1)):
        if what:
            parts = [(pl.ds(0, words), pl.ds(0, t))]
        else:
            parts = [(pl.ds(0, low), pl.ds(0, t)), (pl.ds(low, words - low), pl.ds(half, half))]
        copies[slot] = []
        for rows, cols in parts:
            copies[slot].append(send(
                own.at[what, rows, cols], halo.at[slot, rows, cols],
                send_sems.at[sem], recv_sems.at[sem], near[by],
            ))
            sem += 1
        for piece in copies[slot]:
            piece.start()

    def arrive(slot):
        for piece in copies[slot]:
            piece.wait_recv()

    W, A = pl.ds(0, t), pl.ds(t, t)
    unpack_across(own.at[1], h1.at[:, A], v.at[W, :])
    unpack_within(own.at[0], eye, tri, h1.at[:, W], vm.at[A, :])
    transpose(eye, v.at[W, :], at)
    psum_in[...] = dot_nt(h1[...], h1[...])
    next_out[...] = dot_nt(at[...], at[...])
    psum_btw[...] = dot_nn(h1[:, W], v[W, :])
    k_load.wait()
    thresh = (k_smem[0] - 2).astype(F32)

    arrive(2)
    unpack_across(halo.at[2], hm_out.at[:, A], vm.at[W, :])
    transpose(eye, vm.at[W, :], atm)
    old_w, new_w = keep(psum_in[...] + dot_nt(atm[...], atm[...]), thresh, h1[:, W])
    w0_out[...] = new_w.astype(F8)
    arrive(1)
    unpack_within(halo.at[1], eye, tri, hm_out.at[:, W])
    _, new = keep(dot_nn(hm_out[...], vm[...]), thresh, hm_out[:, A])
    am_out[...] = new.astype(F8)
    arrive(3)
    unpack_within(halo.at[3], eye, tri, w1_out, v.at[A, :])
    old_a, new_a = keep(psum_btw[...] + dot_nn(h1[:, A], v[A, :]), thresh, h1[:, A])
    a0_out[...] = new_a.astype(F8)
    cnt_out[...] = removed(old_w, new_w, old_a, new_a)
    for i, slot in enumerate((0, 4, 5)):
        arrive(slot)
        late[i] = halo[slot]
    for pieces in copies.values():
        for piece in pieces:
            piece.wait_send()


def second(
    n, k_ref, late, hm, w1, am, w0, a0, psum_next, cnt1,
    out_ref, cnt_ref,
    k_smem, spare, atm, h2, v2, g0, u0, g1, u1, g2, at0, at1, r1, q1, at2, eye, tri,
    mine, mine2, row_in, col_in,
    k_sem, row_send, row_recv, col_send, col_recv,
):
    t = w1.shape[0]
    me = lax.axis_index("rows")
    rows = n // ROW
    place, line = lax.rem(me, ROW), lax.div(me, ROW)
    barrier = pltpu.get_barrier_semaphore()

    def beside(d):
        return line * ROW + lax.rem(place + d, ROW)

    def across(d):
        return lax.rem(line + d, rows) * ROW + place

    def greet_row(d, carry):
        greet(barrier, beside(d))
        return carry

    def greet_col(d, carry):
        greet(barrier, across(d))
        return carry

    lax.fori_loop(1, rows, greet_col, 0)
    lax.fori_loop(1, ROW, greet_row, 0)
    k_load = pltpu.make_async_copy(k_ref, k_smem, k_sem)
    k_load.start()
    set_eye(eye)
    W, A = pl.ds(0, t), pl.ds(t, t)

    unpack_across(late.at[0], spare)
    transpose(eye, spare, atm)
    h2[:, W] = w1[...]
    unpack_across(late.at[1], h2.at[:, A], v2.at[W, :])
    unpack_within(late.at[2], eye, tri, v2.at[A, :])
    k_load.wait()
    thresh = (k_smem[0] - 2).astype(F32)

    _, new = keep(dot_nt(hm[...], hm[...]) + dot_nt(atm[...], atm[...]), thresh, hm[:, W])
    g0[:, W] = new.astype(F8)
    g0[:, A] = am[...]
    u0[W, :] = am[...]
    u0[A, :] = w0[...]
    g1[:, W] = w0[...]
    g1[:, A] = a0[...]
    u1[W, :] = a0[...]
    transpose(eye, am, at0)
    transpose(eye, a0, at1)
    _, new = keep(psum_next[...] + dot_nt(h2[...], h2[...]), thresh, w1[...])
    u1[A, :] = new.astype(F8)
    g2[:, W] = new.astype(F8)
    _, new = keep(dot_nn(h2[...], v2[...]), thresh, h2[:, A])
    g2[:, A] = new.astype(F8)

    _, new = keep(dot_nn(g0[...], u0[...]), thresh, g0[:, A])
    spare[...] = new.astype(F8)
    old_w, new_w = keep(dot_nt(at0[...], at0[...]) + dot_nt(g1[...], g1[...]), thresh, g1[:, W])
    r1[:, W] = new_w.astype(F8)
    old_a, new_a = keep(dot_nn(g1[...], u1[...]), thresh, g1[:, A])
    r1[:, A] = new_a.astype(F8)
    q1[W, :] = new_a.astype(F8)
    cnt2 = removed(old_w, new_w, old_a, new_a)
    transpose(eye, spare, at2)
    _, new = keep(dot_nt(at1[...], at1[...]) + dot_nt(g2[...], g2[...]), thresh, g2[:, W])
    q1[A, :] = new.astype(F8)

    support_w = dot_nt(at2[...], at2[...]) + dot_nt(r1[...], r1[...])
    old_w, new_w = keep(support_w, thresh, r1[:, W])
    out_ref[:, W] = support_w * new_w
    support_a = dot_nn(r1[...], q1[...])
    old_a, new_a = keep(support_a, thresh, r1[:, A])
    out_ref[:, A] = support_a * new_a
    lane = lax.broadcasted_iota(jnp.int32, (1, 128), 1)
    packed = jnp.zeros((1, 128), F32)
    for step, row in enumerate((cnt1[...], cnt2, removed(old_w, new_w, old_a, new_a))):
        packed = jnp.where(lane == step, jnp.sum(row, axis=1, keepdims=True), packed)
    mine[...] = packed.astype(jnp.int32)
    pl.semaphore_wait(barrier, rows + ROW - 2)

    def share_row(d, carry):
        send(mine, row_in.at[d - 1], row_send, row_recv, beside(d)).start()
        return carry

    def share_col(d, carry):
        send(mine2, col_in.at[d - 1], col_send, col_recv, across(d)).start()
        return carry

    lax.fori_loop(1, ROW, share_row, 0)
    pltpu.make_async_copy(row_in, row_in, row_recv).wait()
    mine2[...] = mine[...] + jnp.sum(row_in[...], axis=0)
    lax.fori_loop(1, rows, share_col, 0)
    pltpu.make_async_copy(row_in, row_in, row_send).wait()
    pltpu.make_async_copy(col_in, col_in, col_recv).wait()
    cnt_ref[...] = mine2[...] + jnp.sum(col_in[...], axis=0)
    pltpu.make_async_copy(col_in, col_in, col_send).wait()


def finish(support_ref, cnt_ref, out_ref, removed_ref, sums, sems, sum_sem):
    parts = sems.shape[0]
    rows = support_ref.shape[0] // parts
    copies = [
        pltpu.make_async_copy(
            support_ref.at[pl.ds(i * rows, rows)], out_ref.at[pl.ds(i * rows, rows)], sems.at[i]
        )
        for i in range(parts)
    ]
    for copy in copies:
        copy.start()
    lane = lax.broadcasted_iota(jnp.int32, cnt_ref.shape, 1)
    for step in range(ITERS):
        sums[step] = jnp.sum(jnp.where(lane == step, cnt_ref[...], 0)) // 2
    last = pltpu.make_async_copy(sums, removed_ref, sum_sem)
    last.start()
    for copy in copies:
        copy.wait()
    last.wait()


def on_device(n, adj_diag, adj_right, alive_diag, alive_right, truss_k):
    words, t = adj_diag.shape
    half = t // 2
    vmem = pl.BlockSpec(memory_space=pltpu.VMEM)
    hbm = pl.BlockSpec(memory_space=pltpu.HBM)
    args = [
        pltpu.with_memory_space_constraint(v, pltpu.HBM)
        for v in (adj_diag, adj_right, alive_diag, alive_right)
    ]
    dma = pltpu.SemaphoreType.DMA
    tile, wide, tall = (pltpu.VMEM(s, F8) for s in ((t, t), (t, 2 * t), (2 * t, t)))
    f32 = pltpu.VMEM((t, t), F32)
    row = pltpu.VMEM((1, 128), jnp.int32)
    eye, tri = pltpu.VMEM((half, half), F8), pltpu.VMEM((t, half), F8)
    shape = jax.ShapeDtypeStruct
    parts = pl.pallas_call(
        functools.partial(first, n),
        out_shape=(
            shape((3, words, t), jnp.int32),
            shape((t, 2 * t), F8),
            shape((t, t), F8),
            shape((t, t), F8),
            shape((t, t), F8),
            shape((t, t), F8),
            shape((t, t), F32),
            shape((1, 128), F32),
        ),
        in_specs=[hbm] * 5,
        out_specs=(vmem,) * 8,
        scratch_shapes=[
            pltpu.SMEM((1,), jnp.int32),
            pltpu.VMEM((4, words, t), jnp.int32),
            pltpu.VMEM((2, words, t), jnp.int32),
            pltpu.VMEM((6, words, t), jnp.int32),
            wide, tall, tall, tile, tile, eye, tri, f32, f32,
            dma, dma((4,)), dma((9,)), dma((9,)),
        ],
        compiler_params=pltpu.CompilerParams(collective_id=0, has_side_effects=True, vmem_limit_bytes=24 * 2**20),
    )(truss_k, *args)
    support, counts = pl.pallas_call(
        functools.partial(second, n),
        out_shape=(shape((t, 2 * t), F32), shape((1, 128), jnp.int32)),
        in_specs=[hbm] + [vmem] * 8,
        out_specs=(vmem, vmem),
        scratch_shapes=[
            pltpu.SMEM((1,), jnp.int32),
            tile, tile, wide, tall, wide, tall, wide, tall, wide, tile, tile, wide, tall, tile, eye, tri,
            row, row,
            pltpu.VMEM((ROW - 1, 1, 128), jnp.int32),
            pltpu.VMEM((n // ROW - 1, 1, 128), jnp.int32),
            dma, dma, dma, dma, dma,
        ],
        compiler_params=pltpu.CompilerParams(collective_id=1, has_side_effects=True, vmem_limit_bytes=24 * 2**20),
    )(truss_k, *parts)
    return pl.pallas_call(
        finish,
        out_shape=(shape((t, 2 * t), F32), shape((ITERS,), jnp.int32)),
        in_specs=[vmem, vmem],
        out_specs=(hbm, hbm),
        scratch_shapes=[pltpu.SMEM((ITERS,), jnp.int32), dma((16,)), dma],
        compiler_params=pltpu.CompilerParams(vmem_limit_bytes=2**20),
    )(support, counts)


def solution(mesh):
    row = P("rows", None)
    return jax.shard_map(
        functools.partial(on_device, mesh.shape["rows"]),
        mesh=mesh,
        in_specs=(row, row, row, row, P()),
        out_specs=(row, P()),
        check_vma=False,
    )
```
